32 devices in a mesh: group: 4 (over x, core), bl: 8 (over z, y).
Axes of the slice: x: 2, y: 2, z: 4, core: 2. Of those that a mesh axis runs over, the one named last changes fastest.
Arguments:
- visibilities: float32 [2, 512, 16, 1024], P(None, ('group', 'bl')), parts along dimension 1, may hold values from -400 to 400
- flags: int32 [512, 8], P(('group', 'bl')), parts along dimension 0, may hold values 0 or 1
Outputs:
- cross_power: float32 [32, 512, 128], P(None, ('group', 'bl')), parts along dimension 1
- bandpower: float32 [128], P('group'), parts along dimension 0
The draws below stay inside these ranges and needn't reach their ends.
There are 4 independent parts, one for each index of `group`. The reference program is written for one: setup_inputs(seed, part) draws one part's arguments, and reference() takes and returns one part's arrays. A program takes and returns all parts, laid end to end along the dimension named above; each array names one. Nothing has to cross between parts.
All inputs are finite; a program needn't handle non-finite values. No bound on the sum of `flags` on one device may be relied on, other than what follows from the above.
Results may differ from the reference program's by a relative error of at most 0.004.
Values may be sent and summed in bfloat16 or wider, within the bound.
A program may use at most 192 MiB of HBM per device.

```python
import math
import jax
import jax.numpy as jnp
from jax import lax

NF = 1024
NT = 16
CB = 128
BW = 32
BL = 128
NCB = 8


def taper_curve():
    angle = jnp.arange(NF, dtype=jnp.int32).astype(jnp.float32) * (2.0 * math.pi / (NF - 1))
    return 0.35875 - 0.48829 * jnp.cos(angle) + 0.14128 * jnp.cos(2.0 * angle) - 0.01168 * jnp.cos(3.0 * angle)


def draw_visibilities(key, part):
    noise_key = jax.random.fold_in(key, 11)
    shape = (2, BL, NT, NF)
    floor_level = 0.01
    noise = jax.random.truncated_normal(noise_key, -6.0, 6.0, shape, jnp.float32)
    envelope = 0.6 * (1.0 + floor_level) / (taper_curve() + floor_level)
    return (noise * envelope[None, None, None, :]).astype(jnp.float32)


def plant(values, rng, smallest, high):
    extent = values.shape
    place = [jax.random.randint(jax.random.fold_in(rng, axis), (), 0, extent[axis]) for axis in range(len(extent))]
    values = values.at[tuple(place)].set(smallest)
    longest = extent.index(max(extent))
    place[longest] = (place[longest] + 1) % extent[longest]
    return values.at[tuple(place)].set(high)


def setup_inputs(seed: int = 0, part: int = 0) -> dict:
    key_list = jax.random.split(jax.random.key(seed), 3)
    part_keys = jax.random.split(jax.random.fold_in(key_list[2], part), 3)
    visibilities = draw_visibilities(jax.random.fold_in(jax.random.fold_in(key_list[2], part), 71), part)
    flags = plant((jax.random.randint(part_keys[1], (BL, NCB), 0, 8) < 7).astype(jnp.int32), jax.random.fold_in(part_keys[1], 1), 0, 1)
    return dict(visibilities=visibilities, flags=flags)


def make_taper():
    angle = jnp.arange(NF, dtype=jnp.int32).astype(jnp.float32) * (2.0 * math.pi / (NF - 1))
    return 0.35875 - 0.48829 * jnp.cos(angle) + 0.14128 * jnp.cos(2.0 * angle) - 0.01168 * jnp.cos(3.0 * angle)

def make_tables():
    index = jnp.arange(NF, dtype=jnp.int32)
    phase = index[:, None] * index[None, :] % NF
    angle = phase.astype(jnp.float32) * (2.0 * math.pi / NF)
    return (jnp.cos(angle), jnp.sin(angle))

def delay_spectra(visibilities, flags):
    count = visibilities.shape[1]
    keep = jnp.broadcast_to(flags[:, :, None], (count, NF // CB, CB)).reshape(count, NF).astype(jnp.float32)
    weight = keep * make_taper()[None, :]
    tapered = visibilities * weight[None, :, None, :]
    real_rows = tapered[0].reshape(count * NT, NF)
    imag_rows = tapered[1].reshape(count * NT, NF)
    cosine, sine = make_tables()
    high = lax.Precision.HIGHEST
    scale = 1.0 / math.sqrt(NF)
    real_out = (jnp.dot(real_rows, cosine, precision=high) + jnp.dot(imag_rows, sine, precision=high)) * scale
    imag_out = (jnp.dot(imag_rows, cosine, precision=high) - jnp.dot(real_rows, sine, precision=high)) * scale
    stacked = jnp.stack([real_out.reshape(count, NT, NF), imag_out.reshape(count, NT, NF)], 2)
    stacked = stacked.reshape(count, NT, 2, NF // BW, BW).transpose(3, 0, 1, 2, 4)
    return stacked.reshape(NF // BW, count, NT * 2 * BW).astype(jnp.bfloat16)

def reference(visibilities, flags):
    delayed = delay_spectra(visibilities, flags).astype(jnp.float32)
    cross_power = jnp.einsum('kbj,kcj->kbc', delayed, delayed, precision=lax.Precision.HIGHEST) / NT
    self_power = lax.optimization_barrier(jnp.sum(delayed * delayed, axis=2)) / NT
    bandpower = (lax.optimization_barrier(jnp.sum(cross_power, axis=(1, 2))) - lax.optimization_barrier(jnp.sum(self_power, axis=1))) / visibilities.shape[1]
    return (cross_power, bandpower)
```

```python
import functools
import math

import jax
import jax.numpy as jnp
import numpy as np
from jax import lax
from jax.experimental import pallas as pl
from jax.experimental.pallas import tpu as pltpu
from jax.sharding import PartitionSpec as P

BW = 32
LANES = 128
CHUNKS = 4
MESH = pl.DeviceIdType.MESH
F32 = jnp.float32
BF16 = jnp.bfloat16


def tables(nf, nt):
    radix = nf // LANES
    a = 2.0 * np.pi / (nf - 1) * np.arange(nf)
    taper = 0.35875 - 0.48829 * np.cos(a) + 0.14128 * np.cos(2 * a) - 0.01168 * np.cos(3 * a)
    n = np.arange(LANES)
    angle = 2.0 * np.pi * np.outer(np.arange(radix), n) / nf
    twiddle = np.concatenate([np.cos(angle), -np.sin(angle)], 0)
    phase = 2.0 * np.pi * (np.outer(n, n) % LANES) / LANES
    c, s = np.cos(phase), np.sin(phase)
    scale = 1.0 / math.sqrt(nf * nt)
    table = np.block([[c, -s], [s, c]]) * scale
    high = table.astype(np.float32).astype(jnp.bfloat16)
    low = (table - high.astype(np.float64)).astype(np.float32).astype(jnp.bfloat16)
    return (
        taper.reshape(radix, LANES).astype(np.float32),
        twiddle.astype(np.float32),
        high,
        low,
    )


def turn(value, k, size):
    re, im = value
    if k == 0:
        return value
    if 4 * k == size:
        return im, -re
    if 8 * k == size:
        h = math.sqrt(0.5)
        return (re + im) * h, (im - re) * h
    if 8 * k == 3 * size:
        h = math.sqrt(0.5)
        return (im - re) * h, (re + im) * -h
    c, s = math.cos(2 * math.pi * k / size), math.sin(2 * math.pi * k / size)
    return re * c + im * s, im * c - re * s


def short_dft(values):
    size = len(values)
    if size == 1:
        return values
    even, odd = short_dft(values[0::2]), short_dft(values[1::2])
    odd = [turn(v, k, size) for k, v in enumerate(odd)]
    low = [(a + c, b + d) for (a, b), (c, d) in zip(even, odd)]
    high = [(a - c, b - d) for (a, b), (c, d) in zip(even, odd)]
    return low + high


def swap_groups(parts):
    n = len(parts)
    width = LANES // n
    lane = lax.broadcasted_iota(jnp.int32, parts[0].shape, 1)
    bit = 1
    while bit < n:
        upper = (lane // (width * bit)) % 2 == 1
        fresh = list(parts)
        for i in range(n):
            if i & bit:
                continue
            j = i | bit
            fresh[i] = jnp.where(upper, pltpu.roll(parts[j], width * bit, 1), parts[i])
            fresh[j] = jnp.where(upper, parts[j], pltpu.roll(parts[i], LANES - width * bit, 1))
        parts = fresh
        bit *= 2
    return parts


def kernel(
    n, vis, flags, taper, twiddle, high, low, cross, band,
    x, zhi, zlo, spec, send, recv, gram, back, home,
    in_sem, send_sem, recv_sem, own_sem, back_sem, home_sem, last_sem,
):
    _, count, nt, nf = vis.shape
    radix = nf // LANES
    bands = nf // BW // n
    total = n * count
    depth = recv.shape[1]
    piece = depth // CHUNKS
    steps = nt // CHUNKS
    half = nt // 2
    me = lax.axis_index("bl")
    order = sorted(range(1, n), key=lambda k: -min(k, n - k))

    def fetch(h, p, q):
        return pltpu.make_async_copy(
            vis.at[p, :, pl.ds(h * half, half), pl.ds(q * LANES, LANES)],
            x.at[p, q, :, pl.ds(h * half, half), :],
            in_sem.at[h, p, q],
        )

    places = [(p, q) for p in range(2) for q in range(radix)]
    for h in range(2):
        for p, q in places:
            fetch(h, p, q).start()

    barrier = pltpu.get_barrier_semaphore()
    for k in order:
        pl.semaphore_signal(
            barrier, inc=1, device_id={"bl": lax.rem(me + k, n)}, device_id_type=MESH
        )

    rows_view = x.reshape(2 * radix * count * nt, LANES)

    def forward(c, peer, slot):
        return pltpu.make_async_remote_copy(
            src_ref=send.at[peer, :, pl.ds(pl.multiple_of(c * piece, LANES), piece)],
            dst_ref=recv.at[
                pl.ds(pl.multiple_of(slot * count, count), count),
                pl.ds(pl.multiple_of(c * piece, LANES), piece),
            ],
            send_sem=send_sem.at[c, peer],
            recv_sem=recv_sem.at[c, slot],
            device_id={"bl": peer},
            device_id_type=MESH,
        )

    def own(c):
        columns = pl.ds(pl.multiple_of(c * piece, LANES), piece)
        return pltpu.make_async_copy(
            send.at[me, :, columns],
            recv.at[pl.ds(pl.multiple_of(me * count, count), count), columns],
            own_sem.at[c],
        )

    def produce(c):
        keep = flags[...].astype(F32)
        weights = [keep[:, q : q + 1] * taper[q : q + 1, :] for q in range(radix)]
        for s in range(steps):
            t = c * steps + s
            values = []
            for q in range(radix):
                pair = [
                    rows_view[pl.ds((p * radix + q) * count * nt + t, count, stride=nt), :]
                    * weights[q]
                    for p in range(2)
                ]
                values.append(tuple(pair))
            for r, (re, im) in enumerate(short_dft(values)):
                if r:
                    c_r, s_r = twiddle[r : r + 1, :], twiddle[radix + r : radix + r + 1, :]
                    re, im = re * c_r - im * s_r, re * s_r + im * c_r
                z = jnp.concatenate([re, im], 1)
                z_hi = z.astype(BF16)
                at = pl.ds((s * radix + r) * count, count)
                zhi[at, :] = z_hi
                zlo[at, :] = (z - z_hi.astype(F32)).astype(BF16)
        dot = functools.partial(jnp.dot, preferred_element_type=F32)
        spec[...] = (
            dot(zhi[...], high[...]) + dot(zlo[...], high[...]) + dot(zhi[...], low[...])
        )
        blocks = [
            spec[pl.ds((s * radix + r) * count, count), pl.ds(p * LANES, LANES)]
            for s in range(steps)
            for p in range(2)
            for r in range(radix)
        ]
        for g in range(len(blocks) // n):
            at = pl.ds(pl.multiple_of(c * piece + g * LANES, LANES), LANES)
            for d, block in enumerate(swap_groups(blocks[g * n : (g + 1) * n])):
                send[d, :, at] = block.astype(BF16)

    def ship(c):
        own(c).start()
        for k in order:
            forward(c, lax.rem(me + k, n), me).start()

    for h in range(2):
        for p, q in places:
            fetch(h, p, q).wait()
        if h == 0:
            produce(0)
            pl.semaphore_wait(barrier, n - 1)
            ship(0)
        first = max(1, h * CHUNKS // 2)

        @pl.loop(first, (h + 1) * CHUNKS // 2)
        def _(c):
            produce(c)
            ship(c)

    lane = lax.broadcasted_iota(jnp.int32, (1, piece), 1)
    group = lane % (LANES // n) // (BW // radix)
    masks = [(group == kb).astype(BF16) for kb in range(bands)]
    gram[...] = jnp.zeros_like(gram)

    @pl.loop(0, CHUNKS)
    def _(c):
        own(c).wait()
        for k in reversed(order):
            peer = lax.rem(me + k, n)
            forward(c, peer, peer).wait_recv()
        block = recv[:, pl.ds(pl.multiple_of(c * piece, LANES), piece)]
        for kb in range(bands):
            gram[kb] += lax.dot_general(
                block, block * masks[kb], (((1,), (1,)), ((), ())), preferred_element_type=F32
            )

    row = lax.broadcasted_iota(jnp.int32, (total, total), 0)
    col = lax.broadcasted_iota(jnp.int32, (total, total), 1)
    spot = lax.broadcasted_iota(jnp.int32, (count, total), 1)
    line = lax.broadcasted_iota(jnp.int32, (count, total), 0)
    extra = jnp.zeros((count, total), F32)
    for kb in range(bands):
        power = gram[kb]
        back[:, kb * count : (kb + 1) * count, :] = power.astype(BF16).reshape(n, count, total)
        side = jnp.sum(jnp.where(row != col, power, 0.0), axis=0, keepdims=True)
        side = jnp.sum(side, axis=1, keepdims=True) * (1.0 / total)
        extra += jnp.where(spot == me * bands + kb, side, 0.0)
    rest = extra - extra.astype(BF16).astype(F32)
    extra = jnp.where(line == 0, extra, jnp.where(line == 1, rest, 0.0)).astype(BF16)
    for d in range(n):
        back[d, bands * count :, :] = extra

    def homeward(peer, slot):
        return pltpu.make_async_remote_copy(
            src_ref=back.at[peer],
            dst_ref=home.at[slot],
            send_sem=back_sem.at[peer],
            recv_sem=home_sem.at[slot],
            device_id={"bl": peer},
            device_id_type=MESH,
        )

    stay = pltpu.make_async_copy(back.at[me], home.at[me], last_sem)
    stay.start()
    for k in order:
        homeward(lax.rem(me + k, n), me).start()

    @pl.loop(0, CHUNKS)
    def _(c):
        for k in order:
            peer = lax.rem(me + k, n)
            forward(c, peer, me).wait_send()

    stay.wait()
    for k in reversed(order):
        peer = lax.rem(me + k, n)
        homeward(peer, peer).wait_recv()
    sums = jnp.zeros((count, total), F32)
    for d in range(n):
        for kb in range(bands):
            cross[d * bands + kb] = home[d, kb * count : (kb + 1) * count, :].astype(F32)
        sums += home[d, bands * count :, :].astype(F32)
    band[...] = jnp.sum(sums, axis=0, keepdims=True)
    for k in order:
        homeward(lax.rem(me + k, n), me).wait_send()


def shards(n, visibilities, flags):
    _, count, nt, nf = visibilities.shape
    radix = nf // LANES
    total = n * count
    bands = nf // BW // n
    depth = nt * 2 * nf // n
    consts = [jnp.asarray(v) for v in tables(nf, nt)]
    rows = nt // CHUNKS * radix * count
    vmem = pl.BlockSpec(memory_space=pltpu.VMEM)
    dma = pltpu.SemaphoreType.DMA
    cross, band = pl.pallas_call(
        functools.partial(kernel, n),
        out_shape=[
            jax.ShapeDtypeStruct((nf // BW, count, total), F32),
            jax.ShapeDtypeStruct((1, total), F32),
        ],
        in_specs=[pl.BlockSpec(memory_space=pl.ANY)] + [vmem] * 5,
        out_specs=[vmem, vmem],
        scratch_shapes=[
            pltpu.VMEM((2, radix, count, nt, LANES), F32),
            pltpu.VMEM((rows, 2 * LANES), BF16),
            pltpu.VMEM((rows, 2 * LANES), BF16),
            pltpu.VMEM((rows, 2 * LANES), F32),
            pltpu.VMEM((n, count, depth), BF16),
            pltpu.VMEM((total, depth), BF16),
            pltpu.VMEM((bands, total, total), F32),
            pltpu.VMEM((n, (bands + 1) * count, total), BF16),
            pltpu.VMEM((n, (bands + 1) * count, total), BF16),
            dma((2, 2, radix)),
            dma((CHUNKS, n)),
            dma((CHUNKS, n)),
            dma((CHUNKS,)),
            dma((n,)),
            dma((n,)),
            dma,
        ],
        compiler_params=pltpu.CompilerParams(
            collective_id=0, has_side_effects=True, vmem_limit_bytes=56 * 1024 * 1024
        ),
    )(visibilities, flags, *consts)
    return cross, band[0, : nf // BW]


def solution(mesh):
    return jax.shard_map(
        functools.partial(shards, mesh.shape["bl"]),
        mesh=mesh,
        in_specs=(P(None, ("group", "bl"), None, None), P(("group", "bl"), None)),
        out_specs=(P(None, ("group", "bl"), None), P("group")),
        check_vma=False,
    )
```

```python
import functools
import math

import jax
import jax.numpy as jnp
import numpy as np
from jax import lax
from jax.experimental import pallas as pl
from jax.experimental.pallas import tpu as pltpu
from jax.sharding import PartitionSpec as P

BW = 32
LANES = 128
CHUNKS = 4
MESH = pl.DeviceIdType.MESH
F32 = jnp.float32
BF16 = jnp.bfloat16


def tables(nf, nt):
    radix = nf // LANES
    a = 2.0 * np.pi / (nf - 1) * np.arange(nf)
    taper = 0.35875 - 0.48829 * np.cos(a) + 0.14128 * np.cos(2 * a) - 0.01168 * np.cos(3 * a)
    n = np.arange(LANES)
    angle = 2.0 * np.pi * np.outer(np.arange(radix), n) / nf
    twiddle = np.concatenate([np.cos(angle), -np.sin(angle)], 0)
    phase = 2.0 * np.pi * (np.outer(n, n) % LANES) / LANES
    c, s = np.cos(phase), np.sin(phase)
    scale = 1.0 / math.sqrt(nf * nt)
    table = np.block([[c, -s], [s, c]]) * scale
    high = table.astype(np.float32).astype(jnp.bfloat16)
    low = (table - high.astype(np.float64)).astype(np.float32).astype(jnp.bfloat16)
    return (
        taper.reshape(radix, LANES).astype(np.float32),
        twiddle.astype(np.float32),
        high,
        low,
    )


def turn(value, k, size):
    re, im = value
    if k == 0:
        return value
    if 4 * k == size:
        return im, -re
    if 8 * k == size:
        h = math.sqrt(0.5)
        return (re + im) * h, (im - re) * h
    if 8 * k == 3 * size:
        h = math.sqrt(0.5)
        return (im - re) * h, (re + im) * -h
    c, s = math.cos(2 * math.pi * k / size), math.sin(2 * math.pi * k / size)
    return re * c + im * s, im * c - re * s


def short_dft(values):
    size = len(values)
    if size == 1:
        return values
    even, odd = short_dft(values[0::2]), short_dft(values[1::2])
    odd = [turn(v, k, size) for k, v in enumerate(odd)]
    low = [(a + c, b + d) for (a, b), (c, d) in zip(even, odd)]
    high = [(a - c, b - d) for (a, b), (c, d) in zip(even, odd)]
    return low + high


def swap_groups(parts):
    n = len(parts)
    width = LANES // n
    lane = lax.broadcasted_iota(jnp.int32, parts[0].shape, 1)
    bit = 1
    while bit < n:
        upper = (lane // (width * bit)) % 2 == 1
        fresh = list(parts)
        for i in range(n):
            if i & bit:
                continue
            j = i | bit
            fresh[i] = jnp.where(upper, pltpu.roll(parts[j], width * bit, 1), parts[i])
            fresh[j] = jnp.where(upper, parts[j], pltpu.roll(parts[i], LANES - width * bit, 1))
        parts = fresh
        bit *= 2
    return parts


def kernel(
    n, vis, flags_hbm, curves_hbm, table_hbm, home,
    x, flags, curves, table, weight, zhi, zlo, spec, send, recv, gram, back,
    in_sem, small_sem, send_sem, recv_sem, own_sem, back_sem, home_sem, last_sem,
):
    _, count, nt, nf = vis.shape
    radix = nf // LANES
    bands = nf // BW // n
    total = n * count
    depth = recv.shape[1]
    piece = depth // CHUNKS
    steps = nt // CHUNKS
    half = nt // 2
    me = lax.axis_index("bl")
    order = sorted(range(1, n), key=lambda k: -min(k, n - k))

    barrier = pltpu.get_barrier_semaphore()
    for k in order:
        pl.semaphore_signal(
            barrier, inc=1, device_id={"bl": lax.rem(me + k, n)}, device_id_type=MESH
        )

    def fetch(h, p, q):
        return pltpu.make_async_copy(
            vis.at[p, :, pl.ds(h * half, half), pl.ds(q * LANES, LANES)],
            x.at[p, q, :, pl.ds(h * half, half), :],
            in_sem.at[h, p, q],
        )

    small = [
        pltpu.make_async_copy(source, target, small_sem.at[i])
        for i, (source, target) in enumerate(
            [(flags_hbm, flags), (curves_hbm, curves), (table_hbm, table)]
        )
    ]
    places = [(p, q) for p in range(2) for q in range(radix)]
    for copy in small:
        copy.start()
    for h in range(2):
        for p, q in places:
            fetch(h, p, q).start()

    for copy in small:
        copy.wait()
    diagonal = lax.broadcasted_iota(jnp.int32, (count, count), 0) == lax.broadcasted_iota(
        jnp.int32, (count, count), 1
    )
    for q in range(radix):
        keep = jnp.where(diagonal, flags[q : q + 1, :].astype(F32), 0.0)
        weight[q] = jnp.sum(keep, axis=1, keepdims=True) * curves[q : q + 1, :]

    rows_view = x.reshape(2 * radix * count * nt, LANES)

    def forward(c, peer, slot):
        return pltpu.make_async_remote_copy(
            src_ref=send.at[peer, :, pl.ds(pl.multiple_of(c * piece, LANES), piece)],
            dst_ref=recv.at[
                pl.ds(pl.multiple_of(slot * count, count), count),
                pl.ds(pl.multiple_of(c * piece, LANES), piece),
            ],
            send_sem=send_sem.at[c, peer],
            recv_sem=recv_sem.at[c, slot],
            device_id={"bl": peer},
            device_id_type=MESH,
        )

    def own(c):
        columns = pl.ds(pl.multiple_of(c * piece, LANES), piece)
        return pltpu.make_async_copy(
            send.at[me, :, columns],
            recv.at[pl.ds(pl.multiple_of(me * count, count), count), columns],
            own_sem.at[c],
        )

    def produce(c):
        for s in range(steps):
            t = c * steps + s
            values = []
            for q in range(radix):
                pair = [
                    rows_view[pl.ds((p * radix + q) * count * nt + t, count, stride=nt), :]
                    * weight[q]
                    for p in range(2)
                ]
                values.append(tuple(pair))
            for r, (re, im) in enumerate(short_dft(values)):
                if r:
                    c_r = curves[radix + r : radix + r + 1, :]
                    s_r = curves[2 * radix + r : 2 * radix + r + 1, :]
                    re, im = re * c_r - im * s_r, re * s_r + im * c_r
                z = jnp.concatenate([re, im], 1)
                z_hi = z.astype(BF16)
                at = pl.ds((s * radix + r) * count, count)
                zhi[at, :] = z_hi
                zlo[at, :] = (z - z_hi.astype(F32)).astype(BF16)
        dot = functools.partial(jnp.dot, preferred_element_type=F32)
        spec[...] = (
            dot(zhi[...], table[0]) + dot(zlo[...], table[0]) + dot(zhi[...], table[1])
        )
        blocks = [
            spec[pl.ds((s * radix + r) * count, count), pl.ds(p * LANES, LANES)]
            for s in range(steps)
            for p in range(2)
            for r in range(radix)
        ]
        for g in range(len(blocks) // n):
            at = pl.ds(pl.multiple_of(c * piece + g * LANES, LANES), LANES)
            for d, block in enumerate(swap_groups(blocks[g * n : (g + 1) * n])):
                send[d, :, at] = block.astype(BF16)

    def ship(c):
        own(c).start()
        for k in order:
            forward(c, lax.rem(me + k, n), me).start()

    for h in range(2):
        for p, q in places:
            fetch(h, p, q).wait()
        if h == 0:
            produce(0)
            pl.semaphore_wait(barrier, n - 1)
            ship(0)
        first = max(1, h * CHUNKS // 2)

        @pl.loop(first, (h + 1) * CHUNKS // 2)
        def _(c):
            produce(c)
            ship(c)

    lane = lax.broadcasted_iota(jnp.int32, (1, piece), 1)
    group = lane % (LANES // n) // (BW // radix)
    masks = [(group == kb).astype(BF16) for kb in range(bands)]
    gram[...] = jnp.zeros_like(gram)

    @pl.loop(0, CHUNKS)
    def _(c):
        own(c).wait()
        for k in reversed(order):
            peer = lax.rem(me + k, n)
            forward(c, peer, peer).wait_recv()
        block = recv[:, pl.ds(pl.multiple_of(c * piece, LANES), piece)]
        for kb in range(bands):
            gram[kb] += lax.dot_general(
                block, block * masks[kb], (((1,), (1,)), ((), ())), preferred_element_type=F32
            )

    row = lax.broadcasted_iota(jnp.int32, (total, total), 0)
    col = lax.broadcasted_iota(jnp.int32, (total, total), 1)
    spot = lax.broadcasted_iota(jnp.int32, (count, total), 1)
    line = lax.broadcasted_iota(jnp.int32, (count, total), 0)
    extra = jnp.zeros((count, total), F32)
    for kb in range(bands):
        power = gram[kb]
        back[:, kb * count : (kb + 1) * count, :] = power.astype(BF16).reshape(n, count, total)
        side = jnp.sum(jnp.where(row != col, power, 0.0), axis=0, keepdims=True)
        side = jnp.sum(side, axis=1, keepdims=True) * (1.0 / total)
        extra += jnp.where(spot == me * bands + kb, side, 0.0)
    rest = extra - extra.astype(BF16).astype(F32)
    extra = jnp.where(line == 0, extra, jnp.where(line == 1, rest, 0.0)).astype(BF16)
    for d in range(n):
        back[d, bands * count :, :] = extra

    def homeward(peer, slot):
        return pltpu.make_async_remote_copy(
            src_ref=back.at[peer],
            dst_ref=home.at[slot],
            send_sem=back_sem.at[peer],
            recv_sem=home_sem.at[slot],
            device_id={"bl": peer},
            device_id_type=MESH,
        )

    stay = pltpu.make_async_copy(back.at[me], home.at[me], last_sem)
    stay.start()
    for k in order:
        homeward(lax.rem(me + k, n), me).start()

    @pl.loop(0, CHUNKS)
    def _(c):
        for k in order:
            peer = lax.rem(me + k, n)
            forward(c, peer, me).wait_send()

    stay.wait()
    for k in reversed(order):
        peer = lax.rem(me + k, n)
        homeward(peer, peer).wait_recv()
    for k in order:
        homeward(lax.rem(me + k, n), me).wait_send()


def unpack(bands, home, cross, band):
    n, _, total = home.shape
    count = cross.shape[1]
    sums = jnp.zeros((count, total), F32)
    for d in range(n):
        for kb in range(bands):
            cross[d * bands + kb] = home[d, kb * count : (kb + 1) * count, :].astype(F32)
        sums += home[d, bands * count :, :].astype(F32)
    band[...] = jnp.sum(sums, axis=0, keepdims=True)[:, : n * bands]


def shards(n, visibilities, flags):
    _, count, nt, nf = visibilities.shape
    radix = nf // LANES
    total = n * count
    bands = nf // BW // n
    depth = nt * 2 * nf // n
    taper, twiddle, high, low = tables(nf, nt)
    curves = jnp.asarray(np.concatenate([taper, twiddle], 0))
    table = jnp.asarray(np.stack([high, low]))
    turned = flags.T
    rows = nt // CHUNKS * radix * count
    vmem = pl.BlockSpec(memory_space=pltpu.VMEM)
    anywhere = pl.BlockSpec(memory_space=pl.ANY)
    dma = pltpu.SemaphoreType.DMA
    home = pl.pallas_call(
        functools.partial(kernel, n),
        out_shape=jax.ShapeDtypeStruct((n, (bands + 1) * count, total), BF16),
        in_specs=[pl.BlockSpec(memory_space=pltpu.HBM)] * 4,
        out_specs=anywhere,
        scratch_shapes=[
            pltpu.VMEM((2, radix, count, nt, LANES), F32),
            pltpu.VMEM(turned.shape, turned.dtype),
            pltpu.VMEM(curves.shape, curves.dtype),
            pltpu.VMEM(table.shape, table.dtype),
            pltpu.VMEM((radix, count, LANES), F32),
            pltpu.VMEM((rows, 2 * LANES), BF16),
            pltpu.VMEM((rows, 2 * LANES), BF16),
            pltpu.VMEM((rows, 2 * LANES), F32),
            pltpu.VMEM((n, count, depth), BF16),
            pltpu.VMEM((total, depth), BF16),
            pltpu.VMEM((bands, total, total), F32),
            pltpu.VMEM((n, (bands + 1) * count, total), BF16),
            dma((2, 2, radix)),
            dma((3,)),
            dma((CHUNKS, n)),
            dma((CHUNKS, n)),
            dma((CHUNKS,)),
            dma((n,)),
            dma((n,)),
            dma,
        ],
        compiler_params=pltpu.CompilerParams(
            collective_id=0, has_side_effects=True, vmem_limit_bytes=24 * 1024 * 1024
        ),
    )(visibilities, turned, curves, table)
    cross, band = pl.pallas_call(
        functools.partial(unpack, bands),
        out_shape=[
            jax.ShapeDtypeStruct((nf // BW, count, total), F32),
            jax.ShapeDtypeStruct((1, nf // BW), F32),
        ],
        in_specs=[vmem],
        out_specs=[vmem, vmem],
        compiler_params=pltpu.CompilerParams(vmem_limit_bytes=8 * 1024 * 1024),
    )(home)
    return cross, band.reshape(nf // BW)


def solution(mesh):
    return jax.shard_map(
        functools.partial(shards, mesh.shape["bl"]),
        mesh=mesh,
        in_specs=(P(None, ("group", "bl"), None, None), P(("group", "bl"), None)),
        out_specs=(P(None, ("group", "bl"), None), P("group")),
        check_vma=False,
    )
```

```python
import functools
import math

import jax
import jax.numpy as jnp
import numpy as np
from jax import lax
from jax.experimental import pallas as pl
from jax.experimental.pallas import tpu as pltpu
from jax.sharding import PartitionSpec as P

BW = 32
LANES = 128
CHUNKS = 4
MESH = pl.DeviceIdType.MESH
F32 = jnp.float32
BF16 = jnp.bfloat16


def tables(nf, nt):
    radix = nf // LANES
    a = 2.0 * np.pi / (nf - 1) * np.arange(nf)
    taper = 0.35875 - 0.48829 * np.cos(a) + 0.14128 * np.cos(2 * a) - 0.01168 * np.cos(3 * a)
    n = np.arange(LANES)
    angle = 2.0 * np.pi * np.outer(np.arange(radix), n) / nf
    twiddle = np.concatenate([np.cos(angle), -np.sin(angle)], 0)
    phase = 2.0 * np.pi * (np.outer(n, n) % LANES) / LANES
    c, s = np.cos(phase), np.sin(phase)
    scale = 1.0 / math.sqrt(nf * nt)
    table = np.block([[c, -s], [s, c]]) * scale
    high = table.astype(np.float32).astype(jnp.bfloat16)
    low = (table - high.astype(np.float64)).astype(np.float32).astype(jnp.bfloat16)
    return (
        taper.reshape(radix, LANES).astype(np.float32),
        twiddle.astype(np.float32),
        high,
        low,
    )


def turn(value, k, size):
    re, im = value
    if k == 0:
        return value
    if 4 * k == size:
        return im, -re
    if 8 * k == size:
        h = math.sqrt(0.5)
        return (re + im) * h, (im - re) * h
    if 8 * k == 3 * size:
        h = math.sqrt(0.5)
        return (im - re) * h, (re + im) * -h
    c, s = math.cos(2 * math.pi * k / size), math.sin(2 * math.pi * k / size)
    return re * c + im * s, im * c - re * s


def short_dft(values):
    size = len(values)
    if size == 1:
        return values
    even, odd = short_dft(values[0::2]), short_dft(values[1::2])
    odd = [turn(v, k, size) for k, v in enumerate(odd)]
    low = [(a + c, b + d) for (a, b), (c, d) in zip(even, odd)]
    high = [(a - c, b - d) for (a, b), (c, d) in zip(even, odd)]
    return low + high


def swap_groups(parts):
    n = len(parts)
    width = LANES // n
    lane = lax.broadcasted_iota(jnp.int32, parts[0].shape, 1)
    bit = 1
    while bit < n:
        upper = (lane // (width * bit)) % 2 == 1
        fresh = list(parts)
        for i in range(n):
            if i & bit:
                continue
            j = i | bit
            fresh[i] = jnp.where(upper, pltpu.roll(parts[j], width * bit, 1), parts[i])
            fresh[j] = jnp.where(upper, parts[j], pltpu.roll(parts[i], LANES - width * bit, 1))
        parts = fresh
        bit *= 2
    return parts


def kernel(
    n, vis, flags_hbm, curves_hbm, table_hbm, home,
    x, flags, curves, table, weight, zhi, zlo, spec, send, recv, gram, back,
    in_sem, small_sem, send_sem, recv_sem, own_sem, back_sem, home_sem, last_sem,
):
    _, count, nt, nf = vis.shape
    radix = nf // LANES
    bands = nf // BW // n
    total = n * count
    depth = recv.shape[1]
    piece = depth // CHUNKS
    steps = nt // CHUNKS
    half = nt // 2
    me = lax.axis_index("bl")
    order = sorted(range(1, n), key=lambda k: -min(k, n - k))

    barrier = pltpu.get_barrier_semaphore()
    for k in order:
        pl.semaphore_signal(
            barrier, inc=1, device_id={"bl": lax.rem(me + k, n)}, device_id_type=MESH
        )

    def fetch(h, p, q):
        return pltpu.make_async_copy(
            vis.at[p, :, pl.ds(h * half, half), pl.ds(q * LANES, LANES)],
            x.at[p, q, :, pl.ds(h * half, half), :],
            in_sem.at[h, p, q],
        )

    small = [
        pltpu.make_async_copy(source, target, small_sem.at[i])
        for i, (source, target) in enumerate(
            [(flags_hbm, flags), (curves_hbm, curves), (table_hbm, table)]
        )
    ]
    places = [(p, q) for p in range(2) for q in range(radix)]
    for copy in small:
        copy.start()
    for h in range(2):
        for p, q in places:
            fetch(h, p, q).start()

    for copy in small:
        copy.wait()
    diagonal = lax.broadcasted_iota(jnp.int32, (count, count), 0) == lax.broadcasted_iota(
        jnp.int32, (count, count), 1
    )
    for q in range(radix):
        keep = jnp.where(diagonal, flags[q : q + 1, :].astype(F32), 0.0)
        weight[q] = jnp.sum(keep, axis=1, keepdims=True) * curves[q : q + 1, :]

    rows_view = x.reshape(2 * radix * count * nt, LANES)

    def forward(c, peer, slot):
        return pltpu.make_async_remote_copy(
            src_ref=send.at[peer, :, pl.ds(pl.multiple_of(c * piece, LANES), piece)],
            dst_ref=recv.at[
                pl.ds(pl.multiple_of(slot * count, count), count),
                pl.ds(pl.multiple_of(c * piece, LANES), piece),
            ],
            send_sem=send_sem.at[c, peer],
            recv_sem=recv_sem.at[c, slot],
            device_id={"bl": peer},
            device_id_type=MESH,
        )

    def own(c):
        columns = pl.ds(pl.multiple_of(c * piece, LANES), piece)
        return pltpu.make_async_copy(
            send.at[me, :, columns],
            recv.at[pl.ds(pl.multiple_of(me * count, count), count), columns],
            own_sem.at[c],
        )

    def produce(c):
        for s in range(steps):
            t = c * steps + s
            values = []
            for q in range(radix):
                pair = [
                    rows_view[pl.ds((p * radix + q) * count * nt + t, count, stride=nt), :]
                    * weight[q]
                    for p in range(2)
                ]
                values.append(tuple(pair))
            for r, (re, im) in enumerate(short_dft(values)):
                if r:
                    c_r = curves[radix + r : radix + r + 1, :]
                    s_r = curves[2 * radix + r : 2 * radix + r + 1, :]
                    re, im = re * c_r - im * s_r, re * s_r + im * c_r
                z = jnp.concatenate([re, im], 1)
                z_hi = z.astype(BF16)
                at = pl.ds((s * radix + r) * count, count)
                zhi[at, :] = z_hi
                zlo[at, :] = (z - z_hi.astype(F32)).astype(BF16)
        dot = functools.partial(jnp.dot, preferred_element_type=F32)
        spec[...] = (
            dot(zhi[...], table[0]) + dot(zlo[...], table[0]) + dot(zhi[...], table[1])
        )
        blocks = [
            spec[pl.ds((s * radix + r) * count, count), pl.ds(p * LANES, LANES)]
            for s in range(steps)
            for p in range(2)
            for r in range(radix)
        ]
        for g in range(len(blocks) // n):
            at = pl.ds(pl.multiple_of(c * piece + g * LANES, LANES), LANES)
            for d, block in enumerate(swap_groups(blocks[g * n : (g + 1) * n])):
                send[d, :, at] = block.astype(BF16)

    def ship(c):
        own(c).start()
        for k in order:
            forward(c, lax.rem(me + k, n), me).start()

    for h in range(2):
        for p, q in places:
            fetch(h, p, q).wait()
        if h == 0:
            produce(0)
            pl.semaphore_wait(barrier, n - 1)
            ship(0)
        first = max(1, h * CHUNKS // 2)

        @pl.loop(first, (h + 1) * CHUNKS // 2)
        def _(c):
            produce(c)
            ship(c)

    lane = lax.broadcasted_iota(jnp.int32, (1, piece), 1)
    group = lane % (LANES // n) // (BW // radix)
    masks = [(group == kb).astype(BF16) for kb in range(bands)]
    gram[...] = jnp.zeros_like(gram)

    @pl.loop(0, CHUNKS)
    def _(c):
        own(c).wait()
        for k in reversed(order):
            peer = lax.rem(me + k, n)
            forward(c, peer, peer).wait_recv()
        block = recv[:, pl.ds(pl.multiple_of(c * piece, LANES), piece)]
        for kb in range(bands):
            gram[kb] += lax.dot_general(
                block, block * masks[kb], (((1,), (1,)), ((), ())), preferred_element_type=F32
            )

    row = lax.broadcasted_iota(jnp.int32, (total, total), 0)
    col = lax.broadcasted_iota(jnp.int32, (total, total), 1)
    spot = lax.broadcasted_iota(jnp.int32, (count, total), 1)
    line = lax.broadcasted_iota(jnp.int32, (count, total), 0)
    extra = jnp.zeros((count, total), F32)
    for kb in range(bands):
        power = gram[kb]
        back[:, kb * count : (kb + 1) * count, :] = power.astype(BF16).reshape(n, count, total)
        side = jnp.sum(jnp.where(row != col, power, 0.0), axis=0, keepdims=True)
        side = jnp.sum(side, axis=1, keepdims=True) * (1.0 / total)
        extra += jnp.where(spot == me * bands + kb, side, 0.0)
    rest = extra - extra.astype(BF16).astype(F32)
    extra = jnp.where(line == 0, extra, jnp.where(line == 1, rest, 0.0)).astype(BF16)
    for d in range(n):
        back[d, bands * count :, :] = extra

    def homeward(peer, slot):
        return pltpu.make_async_remote_copy(
            src_ref=back.at[peer],
            dst_ref=home.at[slot],
            send_sem=back_sem.at[peer],
            recv_sem=home_sem.at[slot],
            device_id={"bl": peer},
            device_id_type=MESH,
        )

    stay = pltpu.make_async_copy(back.at[me], home.at[me], last_sem)
    stay.start()
    for k in order:
        homeward(lax.rem(me + k, n), me).start()

    @pl.loop(0, CHUNKS)
    def _(c):
        for k in order:
            peer = lax.rem(me + k, n)
            forward(c, peer, me).wait_send()

    stay.wait()
    for k in reversed(order):
        peer = lax.rem(me + k, n)
        homeward(peer, peer).wait_recv()
    for k in order:
        homeward(lax.rem(me + k, n), me).wait_send()


def unpack(bands, home, cross, band):
    n, _, total = home.shape
    count = cross.shape[1]
    sums = jnp.zeros((count, total), F32)
    for d in range(n):
        for kb in range(bands):
            cross[d * bands + kb] = home[d, kb * count : (kb + 1) * count, :].astype(F32)
        sums += home[d, bands * count :, :].astype(F32)
    band[...] = jnp.sum(sums, axis=0, keepdims=True)[:, : n * bands]


def shards(n, visibilities, flags):
    _, count, nt, nf = visibilities.shape
    radix = nf // LANES
    total = n * count
    bands = nf // BW // n
    depth = nt * 2 * nf // n
    taper, twiddle, high, low = tables(nf, nt)
    curves = jnp.asarray(np.concatenate([taper, twiddle], 0))
    table = jnp.asarray(np.stack([high, low]))
    turned = flags.T
    rows = nt // CHUNKS * radix * count
    vmem = pl.BlockSpec(memory_space=pltpu.VMEM)
    anywhere = pl.BlockSpec(memory_space=pl.ANY)
    dma = pltpu.SemaphoreType.DMA
    home = pl.pallas_call(
        functools.partial(kernel, n),
        out_shape=jax.ShapeDtypeStruct((n, (bands + 1) * count, total), BF16),
        in_specs=[pl.BlockSpec(memory_space=pltpu.HBM)] * 4,
        out_specs=anywhere,
        scratch_shapes=[
            pltpu.VMEM((2, radix, count, nt, LANES), F32),
            pltpu.VMEM(turned.shape, turned.dtype),
            pltpu.VMEM(curves.shape, curves.dtype),
            pltpu.VMEM(table.shape, table.dtype),
            pltpu.VMEM((radix, count, LANES), F32),
            pltpu.VMEM((rows, 2 * LANES), BF16),
            pltpu.VMEM((rows, 2 * LANES), BF16),
            pltpu.VMEM((rows, 2 * LANES), F32),
            pltpu.VMEM((n, count, depth), BF16),
            pltpu.VMEM((total, depth), BF16),
            pltpu.VMEM((bands, total, total), F32),
            pltpu.VMEM((n, (bands + 1) * count, total), BF16),
            dma((2, 2, radix)),
            dma((3,)),
            dma((CHUNKS, n)),
            dma((CHUNKS, n)),
            dma((CHUNKS,)),
            dma((n,)),
            dma((n,)),
            dma,
        ],
        compiler_params=pltpu.CompilerParams(
            collective_id=0, has_side_effects=True, vmem_limit_bytes=56 * 1024 * 1024
        ),
    )(visibilities, turned, curves, table)
    cross, band = pl.pallas_call(
        functools.partial(unpack, bands),
        out_shape=[
            jax.ShapeDtypeStruct((nf // BW, count, total), F32),
            jax.ShapeDtypeStruct((1, nf // BW), F32),
        ],
        in_specs=[vmem],
        out_specs=[vmem, vmem],
        compiler_params=pltpu.CompilerParams(vmem_limit_bytes=8 * 1024 * 1024),
    )(home)
    return cross, band.reshape(nf // BW)


def solution(mesh):
    return jax.shard_map(
        functools.partial(shards, mesh.shape["bl"]),
        mesh=mesh,
        in_specs=(P(None, ("group", "bl"), None, None), P(("group", "bl"), None)),
        out_specs=(P(None, ("group", "bl"), None), P("group")),
        check_vma=False,
    )
```
